8 devices in a mesh: ep: 8 (over z, y, x, core).
Axes of the slice: x: 2, y: 2, z: 1, core: 2. Of those that a mesh axis runs over, the one named last changes fastest.
Arguments:
- hidden: bfloat16 [1024, 2048], P('ep')
- w_router: float32 [2048, 8], replicated
- expert_ids: int32 [1024, 2], P('ep')
- w_one: bfloat16 [8, 2048, 5632], P('ep')
- w_three: bfloat16 [8, 2048, 5632], P('ep')
- w_two: bfloat16 [8, 5632, 2048], P('ep')
Outputs:
- output: bfloat16 [1024, 2048], P('ep')
All inputs are finite; a program needn't handle non-finite values.
Results may differ from the reference program's by a relative error of at most 0.00869076.
Values are sent between devices in bfloat16 or wider.
A program may use at most 1 GiB of HBM per device.

```python
import jax
import jax.numpy as jnp
from jax import lax

TOK_DEV = 128
GROUP = 8
D = 2048
FF = 5632
EXPERTS = 8
ROW_BLOCK = 32


def route_ids(key):
    key_hot, key_src = jax.random.split(key)
    dev_order = jax.random.permutation(key_hot, GROUP)
    n_hot = GROUP // 4
    n_cold = GROUP - n_hot
    row_cap = 4 * TOK_DEV // GROUP
    per_dev = EXPERTS // GROUP
    hot_devs = dev_order[:n_hot]
    cold_devs = dev_order[n_hot:]
    slot_idx = jnp.arange(TOK_DEV)

    def one_source(src_key):
        key_shift, key_first, key_second, key_flip, key_perm = jax.random.split(src_key, 5)
        shift_val = jax.random.randint(key_shift, (), 0, n_cold)
        first_dev = hot_devs[slot_idx // row_cap]
        second_dev = cold_devs[(slot_idx + shift_val) % n_cold]
        first_exp = first_dev * per_dev + jax.random.randint(key_first, (TOK_DEV,), 0, per_dev)
        second_exp = second_dev * per_dev + jax.random.randint(key_second, (TOK_DEV,), 0, per_dev)
        pair_ids = jnp.stack([first_exp, second_exp], axis=1)
        flip_bit = jax.random.randint(key_flip, (TOK_DEV, 1), 0, 2)
        pair_ids = jnp.where(flip_bit == 1, pair_ids[:, ::-1], pair_ids)
        token_perm = jax.random.permutation(key_perm, TOK_DEV)
        return pair_ids[token_perm]

    src_keys = jax.random.split(key_src, GROUP)
    return jax.vmap(one_source)(src_keys).reshape(GROUP * TOK_DEV, 2).astype(jnp.int32)


def setup_inputs(seed: int = 0) -> dict:
    key = jax.random.key(seed)
    key_hidden, key_router, key_ids, key_one, key_three, key_two = jax.random.split(key, 6)
    tok_count = GROUP * TOK_DEV
    hidden = jax.random.normal(key_hidden, (tok_count, D), jnp.float32).astype(jnp.bfloat16)
    w_router = jax.random.normal(key_router, (D, EXPERTS), jnp.float32) * D ** -0.5
    expert_ids = route_ids(key_ids)
    w_one = (jax.random.normal(key_one, (EXPERTS, D, FF), jnp.float32) * D ** -0.5).astype(jnp.bfloat16)
    w_three = (jax.random.normal(key_three, (EXPERTS, D, FF), jnp.float32) * D ** -0.5).astype(jnp.bfloat16)
    w_two = (jax.random.normal(key_two, (EXPERTS, FF, D), jnp.float32) * FF ** -0.5).astype(jnp.bfloat16)
    return {"hidden": hidden, "w_router": w_router, "expert_ids": expert_ids, "w_one": w_one, "w_three": w_three, "w_two": w_two}


def reference(hidden, w_router, expert_ids, w_one, w_three, w_two):
    tok_count = hidden.shape[0]
    model_dim = hidden.shape[1]
    logits = jnp.dot(hidden.astype(jnp.float32), w_router, preferred_element_type=jnp.float32)
    prob_vals = jax.nn.softmax(logits, axis=-1)
    picked = jnp.take_along_axis(prob_vals, expert_ids, axis=1)
    gate_vals = picked / jnp.sum(picked, axis=1, keepdims=True)
    flat_ids = expert_ids.reshape(-1)
    assign_count = flat_ids.shape[0]
    sort_order = jnp.argsort(flat_ids, stable=True)
    sorted_ids = flat_ids[sort_order]
    counts = jnp.zeros((EXPERTS,), jnp.int32).at[flat_ids].add(1)
    padded = (counts + ROW_BLOCK - 1) // ROW_BLOCK * ROW_BLOCK
    pad_end = jnp.cumsum(padded)
    pad_start = pad_end - padded
    first_row = jnp.cumsum(counts) - counts
    rank_in = jnp.arange(assign_count) - first_row[sorted_ids]
    dest_row = pad_start[sorted_ids] + rank_in
    row_total = assign_count + EXPERTS * ROW_BLOCK
    block_count = row_total // ROW_BLOCK
    row_tok = jnp.zeros((row_total,), jnp.int32).at[dest_row].set((sort_order // 2).astype(jnp.int32))
    block_start = jnp.arange(block_count) * ROW_BLOCK
    block_exp = jnp.minimum(jnp.sum((block_start[:, None] >= pad_end[None, :]).astype(jnp.int32), axis=1), EXPERTS - 1)
    hidden_blocks = hidden[row_tok].reshape(block_count, ROW_BLOCK, model_dim)

    def block_ffn(block_args):
        hid_blk, exp_idx = block_args
        h_one = jnp.dot(hid_blk, w_one[exp_idx], preferred_element_type=jnp.float32)
        h_three = jnp.dot(hid_blk, w_three[exp_idx], preferred_element_type=jnp.float32)
        act_rows = (jax.nn.silu(h_one) * h_three).astype(jnp.bfloat16)
        return jnp.dot(act_rows, w_two[exp_idx], preferred_element_type=jnp.float32).astype(jnp.bfloat16)

    out_blocks = lax.map(block_ffn, (hidden_blocks, block_exp))
    out_rows = out_blocks.reshape(row_total, model_dim)
    sorted_out = out_rows[dest_row]
    assign_out = jnp.zeros((assign_count, model_dim), jnp.bfloat16).at[sort_order].set(sorted_out)
    both_out = assign_out.reshape(tok_count, 2, model_dim).astype(jnp.float32)
    out_sum = jnp.sum(gate_vals[:, :, None] * both_out, axis=1)
    return out_sum.astype(jnp.bfloat16)
```

```python
import functools

import jax
import jax.numpy as jnp
from jax import lax
from jax.experimental import pallas as pl
from jax.experimental.pallas import tpu as pltpu
from jax.sharding import PartitionSpec as P

MESH = pl.DeviceIdType.MESH
N_DEV = 8
CAP = 64
TOK = 128
TN = 512
SPLIT = 6
ROW_ORDER = (6, 7, 0, 1, 2, 4, 3, 5)
POS = tuple(ROW_ORDER.index(k) for k in range(N_DEV))
F32 = jnp.float32
BF16 = jnp.bfloat16


def peer_of(me, k):
    for bit in (1, 2, 4):
        if k & bit:
            me = me + bit - 2 * bit * ((me // bit) % 2)
    return me


def dot(a, b):
    return jnp.dot(a, b, preferred_element_type=F32)


def moe_kernel(hid_hbm, router_hbm, ids_hbm, w1_hbm, w3_hbm, w2_hbm, out_hbm,
               hid, router, ids, x, xsend, back, h, pool, keyt,
               in_sem, pool_sem, xs_sem, xr_sem, rs_sem, rr_sem, out_sem):
    me = lax.axis_index("ep")
    d_model = hid.shape[1]
    ff = h.shape[1]
    n_ff = ff // TN
    n_out = d_model // TN
    kparts = [(s, min(d_model, ff - s)) for s in range(0, ff, d_model)]
    n_k = len(kparts)
    w2_home = 2 * n_ff

    ids_copy = pltpu.make_async_copy(ids_hbm, ids, in_sem.at[0])
    hid_copy = pltpu.make_async_copy(hid_hbm, hid, in_sem.at[1])
    router_copy = pltpu.make_async_copy(router_hbm, router, in_sem.at[2])
    ids_copy.start()
    hid_copy.start()

    def up_copies(j):
        cols = pl.ds(pl.multiple_of(j * TN, TN), TN)
        return (pltpu.make_async_copy(w1_hbm.at[0, :, cols], pool.at[2 * j], pool_sem.at[2 * j]),
                pltpu.make_async_copy(w3_hbm.at[0, :, cols], pool.at[2 * j + 1], pool_sem.at[2 * j + 1]))

    def down_copies(n, base):
        cols = pl.ds(pl.multiple_of(n * TN, TN), TN)
        return [pltpu.make_async_copy(w2_hbm.at[0, pl.ds(s, size), cols], pool.at[base + i, pl.ds(0, size), :],
                                      pool_sem.at[base + i]) for i, (s, size) in enumerate(kparts)]

    def start_all(copies):
        for c in copies:
            c.start()

    def wait_all(copies):
        for c in copies:
            c.wait()

    @pl.loop(0, n_ff)
    def _(j):
        start_all(up_copies(j))

    router_copy.start()
    start_all(down_copies(0, w2_home))

    barrier = pltpu.get_barrier_semaphore()
    for k in range(1, N_DEV):
        pl.semaphore_signal(barrier, inc=1, device_id=(peer_of(me, k),), device_id_type=MESH)

    ids_copy.wait()
    lane = lax.broadcasted_iota(jnp.int32, (TOK, TOK), 1)
    row = lax.broadcasted_iota(jnp.int32, (TOK, TOK), 0)
    expert = lax.broadcasted_iota(jnp.int32, (N_DEV, TOK), 0)
    chosen = jnp.where((expert == ids[0:1, :]) | (expert == ids[1:2, :]), 1.0, 0.0)
    before = jnp.where(row < lane, 1.0, 0.0)
    rank = dot(chosen.astype(BF16), before.astype(BF16))
    keyt[...] = jnp.where(chosen > 0.0, rank, -1.0)
    slot = lax.broadcasted_iota(jnp.int32, (CAP, TOK), 0).astype(F32)

    def select(k):
        return jnp.where(slot == keyt[pl.ds(peer_of(me, k), 1), :], 1.0, 0.0).astype(BF16)

    def send_copy(k):
        return pltpu.make_async_remote_copy(
            src_ref=xsend.at[pl.ds((k - 1) * CAP, CAP), :], dst_ref=x.at[pl.ds(POS[k] * CAP, CAP), :],
            send_sem=xs_sem.at[k], recv_sem=xr_sem.at[k], device_id=(peer_of(me, k),), device_id_type=MESH)

    hid_copy.wait()

    def pack(ks):
        pick = jnp.concatenate([select(k) for k in ks], axis=0)
        for n in range(n_out):
            cols = pl.ds(n * TN, TN)
            rows = dot(pick, hid[:, cols]).astype(BF16)
            for i, k in enumerate(ks):
                piece = rows[i * CAP:(i + 1) * CAP]
                if k == 0:
                    x[pl.ds(POS[0] * CAP, CAP), cols] = piece
                else:
                    xsend[pl.ds((k - 1) * CAP, CAP), cols] = piece

    pack((2, 4, 1, 0))
    pl.semaphore_wait(barrier, N_DEV - 1)
    for k in (2, 4, 1):
        send_copy(k).start()
    pack((3, 5, 6, 7))
    for k in (3, 5, 6, 7):
        send_copy(k).start()

    own, near, late, far = 128, 256, 384, 0

    def h_row(r):
        return far if r == late else r

    def up_tile(j, r0, rows):
        xr = x[pl.ds(r0, rows), :]
        half = TN // 2
        for c in range(2):
            cols = pl.ds(c * half, half)
            u = dot(xr, pool[2 * j, :, cols])
            v = dot(xr, pool[2 * j + 1, :, cols])
            act = (jax.nn.silu(u) * v).astype(BF16)
            cols = pl.ds(pl.multiple_of(j * TN + c * half, half), half)
            for i in range(0, rows, 128):
                h[pl.ds(h_row(r0 + i), 128), cols] = act[i:i + 128]

    def return_copy(k, n):
        cols = pl.ds(pl.multiple_of(n * TN, TN), TN)
        return pltpu.make_async_remote_copy(
            src_ref=x.at[pl.ds(POS[k] * CAP, CAP), cols], dst_ref=back.at[pl.ds(k * CAP, CAP), cols],
            send_sem=rs_sem.at[k, n], recv_sem=rr_sem.at[k, n], device_id=(peer_of(me, k),), device_id_type=MESH)

    def down_tile(n, base, r0, rows):
        cols = pl.ds(pl.multiple_of(n * TN, TN), TN)
        acc = None
        for i, (s, size) in enumerate(kparts):
            act = jnp.concatenate([h[pl.ds(h_row(r0 + m), 128), pl.ds(s, size)] for m in range(0, rows, 128)], axis=0)
            part = dot(act, pool[base + i, pl.ds(0, size), :])
            acc = part if acc is None else acc + part
        res = acc.astype(BF16)
        x[pl.ds(r0, rows), cols] = res
        for i in range(rows // CAP):
            k = ROW_ORDER[r0 // CAP + i]
            if k == 0:
                back[pl.ds(0, CAP), cols] = res[i * CAP:(i + 1) * CAP]
            else:
                return_copy(k, n).start()

    send_copy(1).wait_recv()

    @pl.loop(0, SPLIT)
    def _(j):
        wait_all(up_copies(j))
        up_tile(j, own, 128)

    send_copy(2).wait_recv()
    send_copy(4).wait_recv()

    @pl.loop(SPLIT, n_ff)
    def _(j):
        wait_all(up_copies(j))
        up_tile(j, own, 256)

    send_copy(3).wait_recv()
    send_copy(5).wait_recv()

    @pl.loop(0, SPLIT)
    def _(j):
        up_tile(j, near, 256)

    @pl.loop(SPLIT, n_ff)
    def _(j):
        up_tile(j, late, 128)

    start_all(down_copies(1, w2_home - n_k))
    start_all(down_copies(2, w2_home - 2 * n_k))

    @pl.loop(0, n_out)
    def _(n):
        base = w2_home - n_k * (n % 3)
        wait_all(down_copies(n, base))
        down_tile(n, base, near, 256)

        @pl.when(n == 0)
        def _():
            start_all(down_copies(3, w2_home))

    kept = (w2_home - 2 * n_k) // 2

    @pl.loop(kept, n_ff)
    def _(j):
        start_all(up_copies(j))

    start_all(down_copies(0, w2_home))
    send_copy(6).wait_recv()
    send_copy(7).wait_recv()

    @pl.loop(0, kept)
    def _(j):
        up_tile(j, far, 128)

    n_slots = w2_home + n_k
    for n in range(1, n_out):
        start_all(down_copies(n, (w2_home + n_k * n) % n_slots))

    @pl.loop(kept, n_ff)
    def _(j):
        wait_all(up_copies(j))
        up_tile(j, far, 128)

    @pl.loop(0, n_out)
    def _(n):
        base = (w2_home + n_k * n) % n_slots
        wait_all(down_copies(n, base))
        down_tile(n, base, far, 256)

    router_copy.wait()
    w = router[...]
    w_hi = w.astype(BF16)
    rest = w - w_hi.astype(F32)
    w_mid = rest.astype(BF16)
    w_lo = (rest - w_mid.astype(F32)).astype(BF16)
    xh = hid[...]

    def logit_part(piece):
        return lax.dot_general(piece, xh, (((1,), (1,)), ((), ())), preferred_element_type=F32)

    logits = (logit_part(w_lo) + logit_part(w_mid)) + logit_part(w_hi)
    ex = jnp.exp(logits - jnp.max(logits, axis=0, keepdims=True))
    prob = ex / jnp.sum(ex, axis=0, keepdims=True)
    gates, wheres = [], []
    for c in range(2):
        hit = expert == ids[c:c + 1, :]
        gates.append(jnp.sum(jnp.where(hit, prob, 0.0), axis=0, keepdims=True))
        r = jnp.sum(jnp.where(hit, keyt[...], 0.0), axis=0, keepdims=True)
        wheres.append((ids[c:c + 1, :] ^ me).astype(F32) * float(CAP) + r)
    total = gates[0] + gates[1]
    cols4 = jnp.concatenate([gates[0] / total, gates[1] / total, wheres[0], wheres[1]]
                            + [jnp.zeros((TOK - 4, TOK), F32)], axis=0).T
    g0, g1 = cols4[:, 0:1], cols4[:, 1:2]

    wide = lax.broadcasted_iota(jnp.int32, (TOK, N_DEV * CAP), 1).astype(F32)
    pick = jnp.concatenate([jnp.where(wide == cols4[:, 2 + c:3 + c], 1.0, 0.0).astype(BF16) for c in range(2)],
                           axis=0)

    out_copies = []
    for n in range(n_out):
        cols = pl.ds(n * TN, TN)
        for k in range(1, N_DEV):
            return_copy(k, n).wait_recv()
        both = dot(pick, back[:, cols])
        hid[:, cols] = (g0 * both[:TOK] + g1 * both[TOK:]).astype(BF16)
        c = pltpu.make_async_copy(hid.at[:, cols], out_hbm.at[:, cols], out_sem.at[n])
        c.start()
        out_copies.append(c)
    for k in range(1, N_DEV):
        send_copy(k).wait_send()
        for n in range(n_out):
            return_copy(k, n).wait_send()
    wait_all(out_copies)


def solution(mesh):
    def device_body(hidden, w_router, ids, w_one, w_three, w_two):
        d_model, ff = w_one.shape[1:]
        n_exp = w_router.shape[1]
        rows = N_DEV * CAP
        n_out = d_model // TN
        n_slots = 2 * (ff // TN) + -(-ff // d_model)
        dma = pltpu.SemaphoreType.DMA
        return pl.pallas_call(
            moe_kernel,
            out_shape=jax.ShapeDtypeStruct(hidden.shape, BF16),
            in_specs=[pl.BlockSpec(memory_space=pl.ANY)] * 6,
            out_specs=pl.BlockSpec(memory_space=pl.ANY),
            scratch_shapes=[
                pltpu.VMEM((TOK, d_model), BF16),
                pltpu.VMEM((n_exp, d_model), F32),
                pltpu.VMEM((2, TOK), jnp.int32),
                pltpu.VMEM((rows, d_model), BF16),
                pltpu.VMEM((rows - CAP, d_model), BF16),
                pltpu.VMEM((rows, d_model), BF16),
                pltpu.VMEM((rows - 128, ff), BF16),
                pltpu.VMEM((n_slots, d_model, TN), BF16),
                pltpu.VMEM((n_exp, TOK), F32),
                dma((3,)), dma((n_slots,)), dma((N_DEV,)), dma((N_DEV,)),
                dma((N_DEV, n_out)), dma((N_DEV, n_out)), dma((n_out,)),
            ],
            compiler_params=pltpu.CompilerParams(
                collective_id=0, has_side_effects=True, vmem_limit_bytes=67043328),
        )(hidden, w_router.T, ids.T, w_one, w_three, w_two)

    return jax.shard_map(
        device_body, mesh=mesh,
        in_specs=(P("ep", None), P(None, None), P("ep", None), P("ep", None, None), P("ep", None, None), P("ep", None, None)),
        out_specs=P("ep", None), check_vma=False)
```

```python
import functools

import jax
import jax.numpy as jnp
from jax import lax
from jax.experimental import pallas as pl
from jax.experimental.pallas import tpu as pltpu
from jax.sharding import PartitionSpec as P

MESH = pl.DeviceIdType.MESH
N_DEV = 8
CAP = 64
TOK = 128
TN = 512
SPLIT = 6
ROW_ORDER = (6, 7, 0, 1, 2, 4, 3, 5)
POS = tuple(ROW_ORDER.index(k) for k in range(N_DEV))
F32 = jnp.float32
BF16 = jnp.bfloat16


def peer_of(me, k):
    for bit in (1, 2, 4):
        if k & bit:
            me = me + bit - 2 * bit * ((me // bit) % 2)
    return me


def dot(a, b):
    return jnp.dot(a, b, preferred_element_type=F32)


def moe_kernel(hid_hbm, router_hbm, ids_hbm, w1_hbm, w3_hbm, w2_hbm, out_hbm,
               hid, router, ids, x, xsend, back, h, pool, keyt,
               in_sem, pool_sem, xs_sem, xr_sem, rs_sem, rr_sem, out_sem):
    me = lax.axis_index("ep")
    d_model = hid.shape[1]
    ff = h.shape[1]
    n_ff = ff // TN
    n_out = d_model // TN
    kparts = [(s, min(d_model, ff - s)) for s in range(0, ff, d_model)]
    n_k = len(kparts)
    w2_home = 2 * n_ff

    ids_copy = pltpu.make_async_copy(ids_hbm, ids, in_sem.at[0])
    hid_copy = pltpu.make_async_copy(hid_hbm, hid, in_sem.at[1])
    router_copy = pltpu.make_async_copy(router_hbm, router, in_sem.at[2])
    ids_copy.start()
    hid_copy.start()

    def up_copies(j):
        cols = pl.ds(pl.multiple_of(j * TN, TN), TN)
        return (pltpu.make_async_copy(w1_hbm.at[0, :, cols], pool.at[2 * j], pool_sem.at[2 * j]),
                pltpu.make_async_copy(w3_hbm.at[0, :, cols], pool.at[2 * j + 1], pool_sem.at[2 * j + 1]))

    def down_copies(n, base):
        cols = pl.ds(pl.multiple_of(n * TN, TN), TN)
        return [pltpu.make_async_copy(w2_hbm.at[0, pl.ds(s, size), cols], pool.at[base + i, pl.ds(0, size), :],
                                      pool_sem.at[base + i]) for i, (s, size) in enumerate(kparts)]

    def start_all(copies):
        for c in copies:
            c.start()

    def wait_all(copies):
        for c in copies:
            c.wait()

    @pl.loop(0, n_ff)
    def _(j):
        start_all(up_copies(j))

    router_copy.start()
    start_all(down_copies(0, w2_home))

    barrier = pltpu.get_barrier_semaphore()
    for k in range(1, N_DEV):
        pl.semaphore_signal(barrier, inc=1, device_id=(peer_of(me, k),), device_id_type=MESH)

    ids_copy.wait()
    lane = lax.broadcasted_iota(jnp.int32, (TOK, TOK), 1)
    row = lax.broadcasted_iota(jnp.int32, (TOK, TOK), 0)
    expert = lax.broadcasted_iota(jnp.int32, (N_DEV, TOK), 0)
    chosen = jnp.where((expert == ids[0:1, :]) | (expert == ids[1:2, :]), 1.0, 0.0)
    before = jnp.where(row < lane, 1.0, 0.0)
    rank = dot(chosen.astype(BF16), before.astype(BF16))
    keyt[...] = jnp.where(chosen > 0.0, rank, -1.0)
    slot = lax.broadcasted_iota(jnp.int32, (CAP, TOK), 0).astype(F32)

    def select(k):
        return jnp.where(slot == keyt[pl.ds(peer_of(me, k), 1), :], 1.0, 0.0).astype(BF16)

    def send_copy(k):
        return pltpu.make_async_remote_copy(
            src_ref=xsend.at[pl.ds((k - 1) * CAP, CAP), :], dst_ref=x.at[pl.ds(POS[k] * CAP, CAP), :],
            send_sem=xs_sem.at[k], recv_sem=xr_sem.at[k], device_id=(peer_of(me, k),), device_id_type=MESH)

    hid_copy.wait()

    def pack(ks):
        pick = jnp.concatenate([select(k) for k in ks], axis=0)
        for n in range(n_out):
            cols = pl.ds(n * TN, TN)
            rows = dot(pick, hid[:, cols]).astype(BF16)
            for i, k in enumerate(ks):
                piece = rows[i * CAP:(i + 1) * CAP]
                if k == 0:
                    x[pl.ds(POS[0] * CAP, CAP), cols] = piece
                else:
                    xsend[pl.ds((k - 1) * CAP, CAP), cols] = piece

    pack((2, 4, 1, 0))
    pl.semaphore_wait(barrier, N_DEV - 1)
    for k in (2, 4, 1):
        send_copy(k).start()
    pack((3, 5, 6, 7))
    for k in (3, 5):
        send_copy(k).start()

    own, near, late, far = 128, 256, 384, 0

    def h_row(r):
        return far if r == late else r

    def up_tile(j, r0, rows):
        xr = x[pl.ds(r0, rows), :]
        half = TN // 2
        for c in range(2):
            cols = pl.ds(c * half, half)
            u = dot(xr, pool[2 * j, :, cols])
            v = dot(xr, pool[2 * j + 1, :, cols])
            act = (jax.nn.silu(u) * v).astype(BF16)
            cols = pl.ds(pl.multiple_of(j * TN + c * half, half), half)
            for i in range(0, rows, 128):
                h[pl.ds(h_row(r0 + i), 128), cols] = act[i:i + 128]

    def return_copy(k, n):
        cols = pl.ds(pl.multiple_of(n * TN, TN), TN)
        return pltpu.make_async_remote_copy(
            src_ref=x.at[pl.ds(POS[k] * CAP, CAP), cols], dst_ref=back.at[pl.ds(k * CAP, CAP), cols],
            send_sem=rs_sem.at[k, n], recv_sem=rr_sem.at[k, n], device_id=(peer_of(me, k),), device_id_type=MESH)

    def down_tile(n, base, r0, rows):
        cols = pl.ds(pl.multiple_of(n * TN, TN), TN)
        acc = None
        for i, (s, size) in enumerate(kparts):
            act = jnp.concatenate([h[pl.ds(h_row(r0 + m), 128), pl.ds(s, size)] for m in range(0, rows, 128)], axis=0)
            part = dot(act, pool[base + i, pl.ds(0, size), :])
            acc = part if acc is None else acc + part
        res = acc.astype(BF16)
        x[pl.ds(r0, rows), cols] = res
        for i in range(rows // CAP):
            k = ROW_ORDER[r0 // CAP + i]
            if k == 0:
                back[pl.ds(0, CAP), cols] = res[i * CAP:(i + 1) * CAP]
            else:
                return_copy(k, n).start()

    send_copy(1).wait_recv()

    @pl.loop(0, SPLIT)
    def _(j):
        wait_all(up_copies(j))
        up_tile(j, own, 128)

    send_copy(2).wait_recv()
    send_copy(4).wait_recv()

    @pl.loop(SPLIT, n_ff)
    def _(j):
        wait_all(up_copies(j))
        up_tile(j, own, 256)

    for k in (6, 7):
        send_copy(k).start()
    send_copy(3).wait_recv()
    send_copy(5).wait_recv()

    @pl.loop(0, SPLIT)
    def _(j):
        up_tile(j, near, 256)

    @pl.loop(SPLIT, n_ff)
    def _(j):
        up_tile(j, late, 128)

    start_all(down_copies(1, w2_home - n_k))
    start_all(down_copies(2, w2_home - 2 * n_k))

    @pl.loop(0, n_out)
    def _(n):
        base = w2_home - n_k * (n % 3)
        wait_all(down_copies(n, base))
        down_tile(n, base, near, 256)

        @pl.when(n == 0)
        def _():
            start_all(down_copies(3, w2_home))

    kept = (w2_home - 2 * n_k) // 2

    @pl.loop(kept, n_ff)
    def _(j):
        start_all(up_copies(j))

    start_all(down_copies(0, w2_home))
    send_copy(6).wait_recv()
    send_copy(7).wait_recv()

    @pl.loop(0, kept)
    def _(j):
        up_tile(j, far, 128)

    n_slots = w2_home + n_k
    for n in range(1, n_out):
        start_all(down_copies(n, (w2_home + n_k * n) % n_slots))

    @pl.loop(kept, n_ff)
    def _(j):
        wait_all(up_copies(j))
        up_tile(j, far, 128)

    @pl.loop(0, n_out)
    def _(n):
        base = (w2_home + n_k * n) % n_slots
        wait_all(down_copies(n, base))
        down_tile(n, base, far, 256)

    router_copy.wait()
    w = router[...]
    w_hi = w.astype(BF16)
    rest = w - w_hi.astype(F32)
    w_mid = rest.astype(BF16)
    w_lo = (rest - w_mid.astype(F32)).astype(BF16)
    xh = hid[...]

    def logit_part(piece):
        return lax.dot_general(piece, xh, (((1,), (1,)), ((), ())), preferred_element_type=F32)

    logits = (logit_part(w_lo) + logit_part(w_mid)) + logit_part(w_hi)
    ex = jnp.exp(logits - jnp.max(logits, axis=0, keepdims=True))
    prob = ex / jnp.sum(ex, axis=0, keepdims=True)
    gates, wheres = [], []
    for c in range(2):
        hit = expert == ids[c:c + 1, :]
        gates.append(jnp.sum(jnp.where(hit, prob, 0.0), axis=0, keepdims=True))
        r = jnp.sum(jnp.where(hit, keyt[...], 0.0), axis=0, keepdims=True)
        wheres.append((ids[c:c + 1, :] ^ me).astype(F32) * float(CAP) + r)
    total = gates[0] + gates[1]
    cols4 = jnp.concatenate([gates[0] / total, gates[1] / total, wheres[0], wheres[1]]
                            + [jnp.zeros((TOK - 4, TOK), F32)], axis=0).T
    g0, g1 = cols4[:, 0:1], cols4[:, 1:2]

    wide = lax.broadcasted_iota(jnp.int32, (TOK, N_DEV * CAP), 1).astype(F32)
    pick = jnp.concatenate([jnp.where(wide == cols4[:, 2 + c:3 + c], 1.0, 0.0).astype(BF16) for c in range(2)],
                           axis=0)

    out_copies = []
    for n in range(n_out):
        cols = pl.ds(n * TN, TN)
        for k in range(1, N_DEV):
            return_copy(k, n).wait_recv()
        both = dot(pick, back[:, cols])
        hid[:, cols] = (g0 * both[:TOK] + g1 * both[TOK:]).astype(BF16)
        c = pltpu.make_async_copy(hid.at[:, cols], out_hbm.at[:, cols], out_sem.at[n])
        c.start()
        out_copies.append(c)
    for k in range(1, N_DEV):
        send_copy(k).wait_send()
        for n in range(n_out):
            return_copy(k, n).wait_send()
    wait_all(out_copies)


def solution(mesh):
    def device_body(hidden, w_router, ids, w_one, w_three, w_two):
        d_model, ff = w_one.shape[1:]
        n_exp = w_router.shape[1]
        rows = N_DEV * CAP
        n_out = d_model // TN
        n_slots = 2 * (ff // TN) + -(-ff // d_model)
        dma = pltpu.SemaphoreType.DMA
        return pl.pallas_call(
            moe_kernel,
            out_shape=jax.ShapeDtypeStruct(hidden.shape, BF16),
            in_specs=[pl.BlockSpec(memory_space=pl.ANY)] * 6,
            out_specs=pl.BlockSpec(memory_space=pl.ANY),
            scratch_shapes=[
                pltpu.VMEM((TOK, d_model), BF16),
                pltpu.VMEM((n_exp, d_model), F32),
                pltpu.VMEM((2, TOK), jnp.int32),
                pltpu.VMEM((rows, d_model), BF16),
                pltpu.VMEM((rows - CAP, d_model), BF16),
                pltpu.VMEM((rows, d_model), BF16),
                pltpu.VMEM((rows - 128, ff), BF16),
                pltpu.VMEM((n_slots, d_model, TN), BF16),
                pltpu.VMEM((n_exp, TOK), F32),
                dma((3,)), dma((n_slots,)), dma((N_DEV,)), dma((N_DEV,)),
                dma((N_DEV, n_out)), dma((N_DEV, n_out)), dma((n_out,)),
            ],
            compiler_params=pltpu.CompilerParams(
                collective_id=0, has_side_effects=True, vmem_limit_bytes=67043328),
        )(hidden, w_router.T, ids.T, w_one, w_three, w_two)

    return jax.shard_map(
        device_body, mesh=mesh,
        in_specs=(P("ep", None), P(None, None), P("ep", None), P("ep", None, None), P("ep", None, None), P("ep", None, None)),
        out_specs=P("ep", None), check_vma=False)
```

```python
import functools

import jax
import jax.numpy as jnp
from jax import lax
from jax.experimental import pallas as pl
from jax.experimental.pallas import tpu as pltpu
from jax.sharding import PartitionSpec as P

MESH = pl.DeviceIdType.MESH
N_DEV = 8
CAP = 64
TOK = 128
TN = 512
SPLIT = 6
ROW_ORDER = (6, 7, 0, 1, 2, 4, 3, 5)
POS = tuple(ROW_ORDER.index(k) for k in range(N_DEV))
F32 = jnp.float32
BF16 = jnp.bfloat16


def peer_of(me, k):
    for bit in (1, 2, 4):
        if k & bit:
            me = me + bit - 2 * bit * ((me // bit) % 2)
    return me


def dot(a, b):
    return jnp.dot(a, b, preferred_element_type=F32)


def moe_kernel(hid_hbm, router_hbm, ids_hbm, w1_hbm, w3_hbm, w2_hbm, out_hbm,
               hid, router, ids, x, xsend, back, h, pool, keyt,
               in_sem, pool_sem, xs_sem, xr_sem, rs_sem, rr_sem, out_sem):
    me = lax.axis_index("ep")
    d_model = hid.shape[1]
    ff = h.shape[1]
    n_ff = ff // TN
    n_out = d_model // TN
    kparts = [(s, min(d_model, ff - s)) for s in range(0, ff, d_model)]
    n_k = len(kparts)
    w2_home = 2 * n_ff

    ids_copy = pltpu.make_async_copy(ids_hbm, ids, in_sem.at[0])
    hid_copy = pltpu.make_async_copy(hid_hbm, hid, in_sem.at[1])
    router_copy = pltpu.make_async_copy(router_hbm, router, in_sem.at[2])
    ids_copy.start()
    hid_copy.start()

    def up_copies(j):
        cols = pl.ds(pl.multiple_of(j * TN, TN), TN)
        return (pltpu.make_async_copy(w1_hbm.at[0, :, cols], pool.at[2 * j], pool_sem.at[2 * j]),
                pltpu.make_async_copy(w3_hbm.at[0, :, cols], pool.at[2 * j + 1], pool_sem.at[2 * j + 1]))

    def down_copies(n, base):
        cols = pl.ds(pl.multiple_of(n * TN, TN), TN)
        return [pltpu.make_async_copy(w2_hbm.at[0, pl.ds(s, size), cols], pool.at[base + i, pl.ds(0, size), :],
                                      pool_sem.at[base + i]) for i, (s, size) in enumerate(kparts)]

    def start_all(copies):
        for c in copies:
            c.start()

    def wait_all(copies):
        for c in copies:
            c.wait()

    @pl.loop(0, n_ff)
    def _(j):
        start_all(up_copies(j))

    router_copy.start()
    start_all(down_copies(0, w2_home))

    barrier = pltpu.get_barrier_semaphore()
    for k in range(1, N_DEV):
        pl.semaphore_signal(barrier, inc=1, device_id=(peer_of(me, k),), device_id_type=MESH)

    ids_copy.wait()
    lane = lax.broadcasted_iota(jnp.int32, (TOK, TOK), 1)
    row = lax.broadcasted_iota(jnp.int32, (TOK, TOK), 0)
    expert = lax.broadcasted_iota(jnp.int32, (N_DEV, TOK), 0)
    chosen = jnp.where((expert == ids[0:1, :]) | (expert == ids[1:2, :]), 1.0, 0.0)
    before = jnp.where(row < lane, 1.0, 0.0)
    rank = dot(chosen.astype(BF16), before.astype(BF16))
    keyt[...] = jnp.where(chosen > 0.0, rank, -1.0)
    slot = lax.broadcasted_iota(jnp.int32, (CAP, TOK), 0).astype(F32)

    def select(k):
        return jnp.where(slot == keyt[pl.ds(peer_of(me, k), 1), :], 1.0, 0.0).astype(BF16)

    def send_copy(k):
        return pltpu.make_async_remote_copy(
            src_ref=xsend.at[pl.ds((k - 1) * CAP, CAP), :], dst_ref=x.at[pl.ds(POS[k] * CAP, CAP), :],
            send_sem=xs_sem.at[k], recv_sem=xr_sem.at[k], device_id=(peer_of(me, k),), device_id_type=MESH)

    hid_copy.wait()

    def pack(ks):
        pick = jnp.concatenate([select(k) for k in ks], axis=0)
        for n in range(n_out):
            cols = pl.ds(n * TN, TN)
            rows = dot(pick, hid[:, cols]).astype(BF16)
            for i, k in enumerate(ks):
                piece = rows[i * CAP:(i + 1) * CAP]
                if k == 0:
                    x[pl.ds(POS[0] * CAP, CAP), cols] = piece
                else:
                    xsend[pl.ds((k - 1) * CAP, CAP), cols] = piece

    pack((2, 4, 1, 0))
    pl.semaphore_wait(barrier, N_DEV - 1)
    for k in (2, 4, 1):
        send_copy(k).start()
    pack((3, 5, 6, 7))

    group = 128
    far, own, near, late = 0, group, 2 * group, 3 * group

    def up_tile(j, r0, h0, rows):
        xr = x[pl.ds(r0, rows), :]
        half = TN // 2
        for c in range(2):
            cols = pl.ds(c * half, half)
            u = dot(xr, pool[2 * j, :, cols])
            v = dot(xr, pool[2 * j + 1, :, cols])
            h[pl.ds(h0, rows), pl.ds(pl.multiple_of(j * TN + c * half, half), half)] = (
                jax.nn.silu(u) * v).astype(BF16)

    def return_copy(k, n):
        cols = pl.ds(n * TN, TN)
        return pltpu.make_async_remote_copy(
            src_ref=x.at[pl.ds(POS[k] * CAP, CAP), cols], dst_ref=back.at[pl.ds(k * CAP, CAP), cols],
            send_sem=rs_sem.at[k, n], recv_sem=rr_sem.at[k, n], device_id=(peer_of(me, k),), device_id_type=MESH)

    def down_tile(n, base, r0, h0):
        cols = pl.ds(n * TN, TN)
        acc = None
        for i, (s, size) in enumerate(kparts):
            part = dot(h[pl.ds(h0, group), pl.ds(s, size)], pool[base + i, pl.ds(0, size), :])
            acc = part if acc is None else acc + part
        res = acc.astype(BF16)
        x[pl.ds(r0, group), cols] = res
        for i in range(group // CAP):
            k = ROW_ORDER[r0 // CAP + i]
            if k == 0:
                back[pl.ds(0, CAP), cols] = res[i * CAP:(i + 1) * CAP]

    def give_back(n, r0):
        for i in range(group // CAP):
            k = ROW_ORDER[r0 // CAP + i]
            if k:
                return_copy(k, n).start()

    send_copy(1).wait_recv()

    @pl.loop(0, SPLIT - 1)
    def _(j):
        wait_all(up_copies(j))
        up_tile(j, own, 0, group)

    for k in (2, 4):
        send_copy(k).wait_send()
    for k in (6, 7):
        send_copy(k).start()
    wait_all(up_copies(SPLIT - 1))
    up_tile(SPLIT - 1, own, 0, group)
    send_copy(2).wait_recv()
    send_copy(4).wait_recv()

    @pl.loop(SPLIT, n_ff)
    def _(j):
        wait_all(up_copies(j))
        up_tile(j, own, 0, 2 * group)

    q1, q2 = w2_home - n_k, w2_home - 2 * n_k
    start_all(down_copies(1, q1))
    start_all(down_copies(2, q2))

    @pl.loop(0, SPLIT, step=3)
    def _(j):
        for i in range(3):
            up_tile(j + i, near, group, group)

    for k in (3, 5):
        send_copy(k).start()

    def up_slot(s):
        cols = pl.ds((s // 2) * TN, TN)
        return pltpu.make_async_copy((w3_hbm if s % 2 else w1_hbm).at[0, :, cols], pool.at[s], pool_sem.at[s])

    def down_pass(steps, r0):
        for n, base, after in steps:
            wait_all(down_copies(n, base))
            down_tile(n, base, r0, group)
            start_all(after)
            give_back(n, r0)

    down_pass([(0, w2_home, down_copies(3, w2_home)),
               (1, q1, [up_slot(s) for s in range(q1, q1 + n_k)]),
               (2, q2, [up_slot(s) for s in range(q2, q2 + n_k)]),
               (3, w2_home, [])], near)

    send_copy(6).wait_recv()
    send_copy(7).wait_recv()

    @pl.loop(0, 8, step=4)
    def _(j):
        for i in range(4):
            up_tile(j + i, far, group, group)

        @pl.when(j == 0)
        def _():
            start_all(down_copies(1, 0))
            start_all(down_copies(2, n_k))

    wait_all([up_slot(s) for s in range(q2, w2_home)])
    for j in range(8, n_ff):
        up_tile(j, far, group, group)
    down_tile(3, w2_home, far, group)
    start_all(down_copies(0, w2_home))
    give_back(3, far)
    down_pass([(1, 0, [up_slot(s) for s in range(0, n_k)]),
               (2, n_k, [up_slot(s) for s in range(n_k, 2 * n_k)]),
               (0, w2_home, [])], far)

    send_copy(3).wait_recv()
    send_copy(5).wait_recv()
    c1, c2, c3 = 2 * n_k, 3 * n_k, 4 * n_k

    @pl.loop(3, n_ff, step=4)
    def _(j):
        for i in range(4):
            up_tile(j + i, late, group, group)

        @pl.when(j == 3)
        def _():
            start_all(down_copies(1, c1))
            start_all(down_copies(2, c2))

    start_all(down_copies(3, c3))
    wait_all([up_slot(s) for s in range(0, 2 * n_k)])
    for j in range(3):
        up_tile(j, late, group, group)
    down_tile(0, w2_home, late, group)
    give_back(0, late)
    down_pass([(1, c1, []), (2, c2, []), (3, c3, [])], late)

    for n, base in enumerate((w2_home, c1, c2, c3)):
        down_tile(n, base, own, 0)
    for n in range(n_out):
        give_back(n, own)

    router_copy.wait()
    w = router[...]
    w_hi = w.astype(BF16)
    rest = w - w_hi.astype(F32)
    w_mid = rest.astype(BF16)
    w_lo = (rest - w_mid.astype(F32)).astype(BF16)
    xh = hid[...]

    def logit_part(piece):
        return lax.dot_general(piece, xh, (((1,), (1,)), ((), ())), preferred_element_type=F32)

    logits = (logit_part(w_lo) + logit_part(w_mid)) + logit_part(w_hi)
    ex = jnp.exp(logits - jnp.max(logits, axis=0, keepdims=True))
    prob = ex / jnp.sum(ex, axis=0, keepdims=True)
    gates, wheres = [], []
    for c in range(2):
        hit = expert == ids[c:c + 1, :]
        gates.append(jnp.sum(jnp.where(hit, prob, 0.0), axis=0, keepdims=True))
        r = jnp.sum(jnp.where(hit, keyt[...], 0.0), axis=0, keepdims=True)
        wheres.append((ids[c:c + 1, :] ^ me).astype(F32) * float(CAP) + r)
    total = gates[0] + gates[1]
    cols4 = jnp.concatenate([gates[0] / total, gates[1] / total, wheres[0], wheres[1]]
                            + [jnp.zeros((TOK - 4, TOK), F32)], axis=0).T
    g0, g1 = cols4[:, 0:1], cols4[:, 1:2]

    wide = lax.broadcasted_iota(jnp.int32, (TOK, N_DEV * CAP), 1).astype(F32)
    pick = jnp.concatenate([jnp.where(wide == cols4[:, 2 + c:3 + c], 1.0, 0.0).astype(BF16) for c in range(2)],
                           axis=0)

    out_copies = []
    for n in range(n_out):
        cols = pl.ds(n * TN, TN)
        for k in range(1, N_DEV):
            return_copy(k, n).wait_recv()
        both = dot(pick, back[:, cols])
        hid[:, cols] = (g0 * both[:TOK] + g1 * both[TOK:]).astype(BF16)
        c = pltpu.make_async_copy(hid.at[:, cols], out_hbm.at[:, cols], out_sem.at[n])
        c.start()
        out_copies.append(c)
    for k in range(1, N_DEV):
        if k not in (2, 4):
            send_copy(k).wait_send()
        for n in range(n_out):
            return_copy(k, n).wait_send()
    wait_all(out_copies)


def solution(mesh):
    def device_body(hidden, w_router, ids, w_one, w_three, w_two):
        d_model, ff = w_one.shape[1:]
        n_exp = w_router.shape[1]
        rows = N_DEV * CAP
        n_out = d_model // TN
        n_slots = 2 * (ff // TN) + -(-ff // d_model)
        dma = pltpu.SemaphoreType.DMA
        return pl.pallas_call(
            moe_kernel,
            out_shape=jax.ShapeDtypeStruct(hidden.shape, BF16),
            in_specs=[pl.BlockSpec(memory_space=pl.ANY)] * 6,
            out_specs=pl.BlockSpec(memory_space=pl.ANY),
            scratch_shapes=[
                pltpu.VMEM((TOK, d_model), BF16),
                pltpu.VMEM((n_exp, d_model), F32),
                pltpu.VMEM((2, TOK), jnp.int32),
                pltpu.VMEM((rows, d_model), BF16),
                pltpu.VMEM((rows - CAP, d_model), BF16),
                pltpu.VMEM((rows, d_model), BF16),
                pltpu.VMEM((2 * TOK, ff), BF16),
                pltpu.VMEM((n_slots, d_model, TN), BF16),
                pltpu.VMEM((n_exp, TOK), F32),
                dma((3,)), dma((n_slots,)), dma((N_DEV,)), dma((N_DEV,)),
                dma((N_DEV, n_out)), dma((N_DEV, n_out)), dma((n_out,)),
            ],
            compiler_params=pltpu.CompilerParams(
                collective_id=0, has_side_effects=True, vmem_limit_bytes=67043328),
        )(hidden, w_router.T, ids.T, w_one, w_three, w_two)

    return jax.shard_map(
        device_body, mesh=mesh,
        in_specs=(P("ep", None), P(None, None), P("ep", None), P("ep", None, None), P("ep", None, None), P("ep", None, None)),
        out_specs=P("ep", None), check_vma=False)
```

```python
import functools

import jax
import jax.numpy as jnp
from jax import lax
from jax.experimental import pallas as pl
from jax.experimental.pallas import tpu as pltpu
from jax.sharding import PartitionSpec as P

MESH = pl.DeviceIdType.MESH
N_DEV = 8
CAP = 64
TOK = 128
TN = 512
VMEM_BYTES = 67043328
EXTRA = 1
SPLIT = 6
ROW_ORDER = (6, 7, 0, 1, 2, 4, 3, 5)
POS = tuple(ROW_ORDER.index(k) for k in range(N_DEV))
XS = {1: 0, 2: 1, 4: 2, 6: 3, 7: 4, 3: 0, 5: 1}
F32 = jnp.float32
BF16 = jnp.bfloat16


def peer_of(me, k):
    for bit in (1, 2, 4):
        if k & bit:
            me = me + bit - 2 * bit * ((me // bit) % 2)
    return me


def dot(a, b):
    return jnp.dot(a, b, preferred_element_type=F32)


def moe_kernel(hid_hbm, router_hbm, ids_hbm, w1_hbm, w3_hbm, w2_hbm, hid,
               router, ids, x, xsend, back, h, pool, keyt, gate,
               in_sem, pool_sem, xs_sem, xr_sem, rs_sem, rr_sem):
    me = lax.axis_index("ep")
    d_model = hid.shape[1]
    ff = h.shape[1]
    n_ff = ff // TN
    n_out = d_model // TN
    kparts = [(s, min(d_model, ff - s)) for s in range(0, ff, d_model)]
    n_k = len(kparts)
    home = [2 * n_ff + i for i in range(n_k)]
    extra = [home[-1] + 1 + i for i in range(EXTRA)]

    ids_copy = pltpu.make_async_copy(ids_hbm, ids, in_sem.at[0])
    hid_copy = pltpu.make_async_copy(hid_hbm, hid, in_sem.at[1])
    router_copy = pltpu.make_async_copy(router_hbm, router, in_sem.at[2])
    ids_copy.start()
    hid_copy.start()
    router_copy.start()

    def up_copies(j):
        cols = pl.ds(pl.multiple_of(j * TN, TN), TN)
        return (pltpu.make_async_copy(w1_hbm.at[0, :, cols], pool.at[2 * j], pool_sem.at[2 * j]),
                pltpu.make_async_copy(w3_hbm.at[0, :, cols], pool.at[2 * j + 1], pool_sem.at[2 * j + 1]))

    def down_copies(n, slots, first=0):
        cols = pl.ds(n * TN, TN)
        return [pltpu.make_async_copy(w2_hbm.at[0, pl.ds(*kparts[first + i]), cols],
                                      pool.at[p, pl.ds(0, kparts[first + i][1]), :], pool_sem.at[p])
                for i, p in enumerate(slots)]

    def start_all(copies):
        for c in copies:
            c.start()

    def wait_all(copies):
        for c in copies:
            c.wait()

    @pl.loop(0, n_ff)
    def _(j):
        start_all(up_copies(j))

    start_all(down_copies(0, home) + down_copies(1, extra))

    barrier = pltpu.get_barrier_semaphore()
    for k in range(1, N_DEV):
        pl.semaphore_signal(barrier, inc=1, device_id=(peer_of(me, k),), device_id_type=MESH)

    ids_copy.wait()
    lane = lax.broadcasted_iota(jnp.int32, (TOK, TOK), 1)
    row = lax.broadcasted_iota(jnp.int32, (TOK, TOK), 0)
    expert = lax.broadcasted_iota(jnp.int32, (N_DEV, TOK), 0)
    chosen = jnp.where((expert == ids[0:1, :]) | (expert == ids[1:2, :]), 1.0, 0.0)
    before = jnp.where(row < lane, 1.0, 0.0)
    rank = dot(chosen.astype(BF16), before.astype(BF16))
    keyt[...] = jnp.where(chosen > 0.0, rank, -1.0)
    slot = lax.broadcasted_iota(jnp.int32, (CAP, TOK), 0).astype(F32)

    def select(k):
        return jnp.where(slot == keyt[pl.ds(peer_of(me, k), 1), :], 1.0, 0.0).astype(BF16)

    def send_block(k):
        return (hid if k in (3, 5) else xsend), pl.ds(XS[k] * CAP, CAP)

    def send_copy(k):
        buf, block = send_block(k)
        return pltpu.make_async_remote_copy(
            src_ref=buf.at[block, :], dst_ref=x.at[pl.ds(POS[k] * CAP, CAP), :],
            send_sem=xs_sem.at[k], recv_sem=xr_sem.at[k], device_id=(peer_of(me, k),), device_id_type=MESH)

    def pack(ks):
        pick = jnp.concatenate([select(k) for k in ks], axis=0)
        for n in range(n_out):
            cols = pl.ds(n * TN, TN)
            rows = dot(pick, hid[:, cols]).astype(BF16)
            for i, k in enumerate(ks):
                piece = rows[i * CAP:(i + 1) * CAP]
                if k == 0:
                    x[pl.ds(POS[0] * CAP, CAP), cols] = piece
                else:
                    buf, block = send_block(k)
                    buf[block, cols] = piece

    hid_copy.wait()
    pack((2, 4))
    pl.semaphore_wait(barrier, N_DEV - 1)
    for k in (2, 4):
        send_copy(k).start()
    pack((1, 0))
    send_copy(1).start()
    pack((6, 7))

    router_copy.wait()
    w = router[...]
    w_hi = w.astype(BF16)
    rest = w - w_hi.astype(F32)
    w_mid = rest.astype(BF16)
    w_lo = (rest - w_mid.astype(F32)).astype(BF16)
    xh = hid[...]

    def logit_part(piece):
        return lax.dot_general(piece, xh, (((1,), (1,)), ((), ())), preferred_element_type=F32)

    logits = (logit_part(w_lo) + logit_part(w_mid)) + logit_part(w_hi)
    ex = jnp.exp(logits - jnp.max(logits, axis=0, keepdims=True))
    prob = ex / jnp.sum(ex, axis=0, keepdims=True)
    gates, wheres = [], []
    for c in range(2):
        hit = expert == ids[c:c + 1, :]
        gates.append(jnp.sum(jnp.where(hit, prob, 0.0), axis=0, keepdims=True))
        r = jnp.sum(jnp.where(hit, keyt[...], 0.0), axis=0, keepdims=True)
        wheres.append((ids[c:c + 1, :] ^ me).astype(F32) * float(CAP) + r)
    total = gates[0] + gates[1]
    cols4 = jnp.concatenate([gates[0] / total, gates[1] / total, wheres[0], wheres[1]]
                            + [jnp.zeros((TOK - 4, TOK), F32)], axis=0).T
    gate[...] = cols4[:, 0:N_DEV]

    pack((3, 5))

    group = 128
    far, own, near, late = 0, group, 2 * group, 3 * group

    def up_tile(j, r0, h0, rows):
        half = TN // 2
        for c in range(2):
            cols = pl.ds(c * half, half)
            u = dot(x[pl.ds(r0, rows), :], pool[2 * j, :, cols])
            v = dot(x[pl.ds(r0, rows), :], pool[2 * j + 1, :, cols])
            h[pl.ds(h0, rows), pl.ds(pl.multiple_of(j * TN + c * half, half), half)] = (
                jax.nn.silu(u) * v).astype(BF16)

    def return_copy(k, n):
        cols = pl.ds(n * TN, TN)
        return pltpu.make_async_remote_copy(
            src_ref=x.at[pl.ds(POS[k] * CAP, CAP), cols], dst_ref=back.at[pl.ds(k * CAP, CAP), cols],
            send_sem=rs_sem.at[n], recv_sem=rr_sem.at[n], device_id=(peer_of(me, k),), device_id_type=MESH)

    def returned(n):
        blocks = pl.ds(CAP, (N_DEV - 1) * CAP)
        cols = pl.ds(pl.multiple_of(n * TN, TN), TN)
        return pltpu.make_async_remote_copy(
            src_ref=x.at[blocks, cols], dst_ref=back.at[blocks, cols],
            send_sem=rs_sem.at[n], recv_sem=rr_sem.at[n], device_id=(peer_of(me, 1),), device_id_type=MESH)

    def down_tile(n, slots, r0, h0, after=None):
        cols = pl.ds(n * TN, TN)
        acc = None
        for i, (s, size) in enumerate(kparts):
            part = dot(h[pl.ds(h0, group), pl.ds(s, size)], pool[slots[i], pl.ds(0, size), :])
            acc = part if acc is None else acc + part
            if after:
                after[i].start()
        res = acc.astype(BF16)
        x[pl.ds(r0, group), cols] = res
        for i in range(group // CAP):
            k = ROW_ORDER[r0 // CAP + i]
            if k == 0:
                back[pl.ds(0, CAP), cols] = res[i * CAP:(i + 1) * CAP]

    def give_back(n, r0):
        for i in range(group // CAP):
            k = ROW_ORDER[r0 // CAP + i]
            if k:
                return_copy(k, n).start()

    send_copy(1).wait_recv()

    @pl.loop(0, SPLIT - 1)
    def _(j):
        wait_all(up_copies(j))
        up_tile(j, own, 0, group)

    for k in (2, 4):
        send_copy(k).wait_send()
    for k in (6, 7):
        send_copy(k).start()
    wait_all(up_copies(SPLIT - 1))
    up_tile(SPLIT - 1, own, 0, group)
    send_copy(2).wait_recv()
    send_copy(4).wait_recv()

    @pl.loop(SPLIT, n_ff)
    def _(j):
        wait_all(up_copies(j))
        up_tile(j, own, 0, 2 * group)

    def up_slots(slots):
        return [pltpu.make_async_copy((w3_hbm if p % 2 else w1_hbm).at[0, :, pl.ds((p // 2) * TN, TN)],
                                      pool.at[p], pool_sem.at[p]) for p in slots]

    rest = n_k - EXTRA

    def middle_copies(lent):
        return down_copies(1, lent[:rest], EXTRA) + down_copies(2, lent[rest:])

    def start_middle(lent):
        start_all(middle_copies(lent))

    def down_middle(lent, r0):
        wait_all(middle_copies(lent))
        down_tile(1, extra + lent[:rest], r0, group)
        down_tile(2, lent[rest:], r0, group)
        for n in (1, 2):
            give_back(n, r0)

    n_lent = rest + n_k
    back_c = -(-n_lent // 2)
    lent_a = list(range(2 * n_ff - n_lent, 2 * n_ff))
    lent_b = list(range(0, n_lent))
    lent_c = list(range(2 * back_c, 2 * back_c + n_lent))
    last_c = list(range(lent_c[-1] + 1, lent_c[-1] + 1 + n_k))
    start_middle(lent_a)

    @pl.loop(0, SPLIT, step=3)
    def _(j):
        for i in range(3):
            up_tile(j + i, near, group, group)

    for k in (3, 5):
        send_copy(k).start()
    wait_all(down_copies(0, home) + down_copies(1, extra))
    down_tile(0, home, near, group, down_copies(3, home))
    give_back(0, near)
    down_middle(lent_a, near)
    start_all(up_slots(lent_a))
    wait_all(down_copies(3, home))
    down_tile(3, home, near, group)
    give_back(3, near)

    send_copy(6).wait_recv()
    send_copy(7).wait_recv()
    for j in range(0, 4):
        up_tile(j, far, group, group)
    start_middle(lent_b)
    for j in range(4, 8):
        up_tile(j, far, group, group)
    wait_all(up_slots(lent_a))
    for j in range(8, n_ff):
        up_tile(j, far, group, group)
    down_tile(3, home, far, group, down_copies(0, home))
    give_back(3, far)
    down_middle(lent_b, far)
    start_all(up_slots(lent_b))
    wait_all(down_copies(0, home))
    down_tile(0, home, far, group)
    give_back(0, far)

    send_copy(3).wait_recv()
    send_copy(5).wait_recv()
    for j in range(back_c, back_c + 4):
        up_tile(j, late, group, group)
    start_middle(lent_c)
    start_all(down_copies(3, last_c))
    for j in range(back_c + 4, n_ff):
        up_tile(j, late, group, group)
    wait_all(up_slots(lent_b))
    for j in range(back_c):
        up_tile(j, late, group, group)
    down_tile(0, home, late, group)
    give_back(0, late)
    down_middle(lent_c, late)
    wait_all(down_copies(3, last_c))
    down_tile(3, last_c, late, group)
    give_back(3, late)

    own_slots = (home, extra + lent_c[:rest], lent_c[rest:], last_c)
    for n in range(2):
        down_tile(n, own_slots[n], own, 0)
    for k in range(1, N_DEV):
        if k not in (2, 4):
            send_copy(k).wait_send()
    for n in range(2, n_out):
        down_tile(n, own_slots[n], own, 0)
    for n in range(n_out):
        give_back(n, own)

    pick = xsend.at[pl.ds(0, 2 * TOK), pl.ds(0, N_DEV * CAP)]
    wide = lax.broadcasted_iota(jnp.int32, (TOK, N_DEV * CAP), 1).astype(F32)
    for c in range(2):
        pick[pl.ds(c * TOK, TOK), :] = jnp.where(wide == gate[:, 2 + c:3 + c], 1.0, 0.0).astype(BF16)

    @pl.loop(0, n_out)
    def _(n):
        cols = pl.ds(pl.multiple_of(n * TN, TN), TN)
        returned(n).wait_recv()
        both = dot(pick[...], back[:, cols])
        hid[:, cols] = (gate[:, 0:1] * both[:TOK] + gate[:, 1:2] * both[TOK:]).astype(BF16)

    @pl.loop(0, n_out)
    def _(n):
        returned(n).wait_send()


def solution(mesh):
    def device_body(hidden, w_router, ids, w_one, w_three, w_two):
        d_model, ff = w_one.shape[1:]
        n_exp = w_router.shape[1]
        rows = N_DEV * CAP
        n_out = d_model // TN
        n_slots = 2 * (ff // TN) + -(-ff // d_model) + EXTRA
        dma = pltpu.SemaphoreType.DMA
        return pl.pallas_call(
            moe_kernel,
            out_shape=pltpu.VMEM(hidden.shape, BF16),
            in_specs=[pl.BlockSpec(memory_space=pl.ANY)] * 6,
            out_specs=pl.BlockSpec(memory_space=pltpu.VMEM),
            scratch_shapes=[
                pltpu.VMEM((n_exp, d_model), F32),
                pltpu.VMEM((2, TOK), jnp.int32),
                pltpu.VMEM((rows, d_model), BF16),
                pltpu.VMEM((5 * CAP, d_model), BF16),
                pltpu.VMEM((rows, d_model), BF16),
                pltpu.VMEM((2 * TOK, ff), BF16),
                pltpu.VMEM((n_slots, d_model, TN), BF16),
                pltpu.VMEM((n_exp, TOK), F32),
                pltpu.VMEM((TOK, N_DEV), F32),
                dma((3,)), dma((n_slots,)), dma((N_DEV,)), dma((N_DEV,)),
                dma((n_out,)), dma((n_out,)),
            ],
            compiler_params=pltpu.CompilerParams(
                collective_id=0, has_side_effects=True, vmem_limit_bytes=VMEM_BYTES - 2 * hidden.size),
        )(hidden, w_router.T, ids.T, w_one, w_three, w_two)

    return jax.shard_map(
        device_body, mesh=mesh,
        in_specs=(P("ep", None), P(None, None), P("ep", None), P("ep", None, None), P("ep", None, None), P("ep", None, None)),
        out_specs=P("ep", None), check_vma=False)
```

```python
import functools

import jax
import jax.numpy as jnp
from jax import lax
from jax.experimental import pallas as pl
from jax.experimental.pallas import tpu as pltpu
from jax.sharding import PartitionSpec as P

MESH = pl.DeviceIdType.MESH
N_DEV = 8
CAP = 64
TOK = 128
TN = 512
VMEM_BYTES = 67043328
EXTRA = 1
SPLIT = 6
ROW_ORDER = (6, 7, 0, 1, 2, 4, 3, 5)
POS = tuple(ROW_ORDER.index(k) for k in range(N_DEV))
XS = {1: 0, 2: 1, 4: 2, 6: 3, 7: 4, 3: 0, 5: 1}
F32 = jnp.float32
BF16 = jnp.bfloat16


def peer_of(me, k):
    for bit in (1, 2, 4):
        if k & bit:
            me = me + bit - 2 * bit * ((me // bit) % 2)
    return me


def dot(a, b):
    return jnp.dot(a, b, preferred_element_type=F32)


def moe_kernel(hid_hbm, router_hbm, ids_hbm, w1_hbm, w3_hbm, w2_hbm, hid,
               router, ids, x, xsend, back, h, pool, keyt, gate,
               in_sem, pool_sem, xs_sem, xr_sem, rs_sem, rr_sem):
    me = lax.axis_index("ep")
    d_model = hid.shape[1]
    ff = h.shape[1]
    n_ff = ff // TN
    n_out = d_model // TN
    kparts = [(s, min(d_model, ff - s)) for s in range(0, ff, d_model)]
    n_k = len(kparts)
    home = [2 * n_ff + i for i in range(n_k)]
    extra = [home[-1] + 1 + i for i in range(EXTRA)]

    ids_copy = pltpu.make_async_copy(ids_hbm, ids, in_sem.at[0])
    hid_copy = pltpu.make_async_copy(hid_hbm, hid, in_sem.at[1])
    router_copy = pltpu.make_async_copy(router_hbm, router, in_sem.at[2])
    ids_copy.start()
    hid_copy.start()
    router_copy.start()

    def up_copies(j):
        cols = pl.ds(pl.multiple_of(j * TN, TN), TN)
        return (pltpu.make_async_copy(w1_hbm.at[0, :, cols], pool.at[2 * j], pool_sem.at[2 * j]),
                pltpu.make_async_copy(w3_hbm.at[0, :, cols], pool.at[2 * j + 1], pool_sem.at[2 * j + 1]))

    def down_copies(n, slots, first=0):
        cols = pl.ds(n * TN, TN)
        return [pltpu.make_async_copy(w2_hbm.at[0, pl.ds(*kparts[first + i]), cols],
                                      pool.at[p, pl.ds(0, kparts[first + i][1]), :], pool_sem.at[p])
                for i, p in enumerate(slots)]

    def start_all(copies):
        for c in copies:
            c.start()

    def wait_all(copies):
        for c in copies:
            c.wait()

    @pl.loop(0, n_ff)
    def _(j):
        start_all(up_copies(j))

    start_all(down_copies(0, home) + down_copies(1, extra))

    barrier = pltpu.get_barrier_semaphore()
    for k in range(1, N_DEV):
        pl.semaphore_signal(barrier, inc=1, device_id=(peer_of(me, k),), device_id_type=MESH)

    ids_copy.wait()
    lane = lax.broadcasted_iota(jnp.int32, (TOK, TOK), 1)
    row = lax.broadcasted_iota(jnp.int32, (TOK, TOK), 0)
    expert = lax.broadcasted_iota(jnp.int32, (N_DEV, TOK), 0)
    chosen = jnp.where((expert == ids[0:1, :]) | (expert == ids[1:2, :]), 1.0, 0.0)
    before = jnp.where(row < lane, 1.0, 0.0)
    rank = dot(chosen.astype(BF16), before.astype(BF16))
    keyt[...] = jnp.where(chosen > 0.0, rank, -1.0)
    slot = lax.broadcasted_iota(jnp.int32, (CAP, TOK), 0).astype(F32)

    def select(k):
        return jnp.where(slot == keyt[pl.ds(peer_of(me, k), 1), :], 1.0, 0.0).astype(BF16)

    def send_block(k):
        return (hid if k in (3, 5) else xsend), pl.ds(XS[k] * CAP, CAP)

    def send_copy(k):
        buf, block = send_block(k)
        return pltpu.make_async_remote_copy(
            src_ref=buf.at[block, :], dst_ref=x.at[pl.ds(POS[k] * CAP, CAP), :],
            send_sem=xs_sem.at[k], recv_sem=xr_sem.at[k], device_id=(peer_of(me, k),), device_id_type=MESH)

    def pack(ks):
        pick = jnp.concatenate([select(k) for k in ks], axis=0)
        for n in range(n_out):
            cols = pl.ds(n * TN, TN)
            rows = dot(pick, hid[:, cols]).astype(BF16)
            for i, k in enumerate(ks):
                piece = rows[i * CAP:(i + 1) * CAP]
                if k == 0:
                    x[pl.ds(POS[0] * CAP, CAP), cols] = piece
                else:
                    buf, block = send_block(k)
                    buf[block, cols] = piece

    hid_copy.wait()
    pack((2, 4))
    pl.semaphore_wait(barrier, N_DEV - 1)
    for k in (2, 4):
        send_copy(k).start()
    pack((1, 0))
    send_copy(1).start()
    pack((6, 7))

    router_copy.wait()
    w = router[...]
    w_hi = w.astype(BF16)
    rest = w - w_hi.astype(F32)
    w_mid = rest.astype(BF16)
    w_lo = (rest - w_mid.astype(F32)).astype(BF16)
    xh = hid[...]

    def logit_part(piece):
        return lax.dot_general(piece, xh, (((1,), (1,)), ((), ())), preferred_element_type=F32)

    logits = (logit_part(w_lo) + logit_part(w_mid)) + logit_part(w_hi)
    ex = jnp.exp(logits - jnp.max(logits, axis=0, keepdims=True))
    prob = ex / jnp.sum(ex, axis=0, keepdims=True)
    gates, wheres = [], []
    for c in range(2):
        hit = expert == ids[c:c + 1, :]
        gates.append(jnp.sum(jnp.where(hit, prob, 0.0), axis=0, keepdims=True))
        r = jnp.sum(jnp.where(hit, keyt[...], 0.0), axis=0, keepdims=True)
        wheres.append((ids[c:c + 1, :] ^ me).astype(F32) * float(CAP) + r)
    total = gates[0] + gates[1]
    cols4 = jnp.concatenate([gates[0] / total, gates[1] / total, wheres[0], wheres[1]]
                            + [jnp.zeros((TOK - 4, TOK), F32)], axis=0).T
    gate[...] = cols4[:, 0:N_DEV]

    pack((3, 5))

    group = 128
    far, own, near, late = 0, group, 2 * group, 3 * group

    def up_tile(j, r0, h0, rows):
        half = TN // 2
        held = x[pl.ds(r0, rows), :] if rows == group else None
        for c in range(2):
            cols = pl.ds(c * half, half)
            u = dot(x[pl.ds(r0, rows), :] if held is None else held, pool[2 * j, :, cols])
            v = dot(x[pl.ds(r0, rows), :] if held is None else held, pool[2 * j + 1, :, cols])
            h[pl.ds(h0, rows), pl.ds(pl.multiple_of(j * TN + c * half, half), half)] = (
                jax.nn.silu(u) * v).astype(BF16)

    def return_copy(k, n, start=0, width=TN):
        cols = pl.ds(n * TN + start, width)
        return pltpu.make_async_remote_copy(
            src_ref=x.at[pl.ds(POS[k] * CAP, CAP), cols], dst_ref=back.at[pl.ds(k * CAP, CAP), cols],
            send_sem=rs_sem.at[n], recv_sem=rr_sem.at[n], device_id=(peer_of(me, k),), device_id_type=MESH)

    def returned(n):
        blocks = pl.ds(CAP, (N_DEV - 1) * CAP)
        cols = pl.ds(pl.multiple_of(n * TN, TN), TN)
        return pltpu.make_async_remote_copy(
            src_ref=x.at[blocks, cols], dst_ref=back.at[blocks, cols],
            send_sem=rs_sem.at[n], recv_sem=rr_sem.at[n], device_id=(peer_of(me, 1),), device_id_type=MESH)

    def down_tile(n, slots, r0, h0, after=None):
        cols = pl.ds(n * TN, TN)
        acc = None
        for i, (s, size) in enumerate(kparts):
            part = dot(h[pl.ds(h0, group), pl.ds(s, size)], pool[slots[i], pl.ds(0, size), :])
            acc = part if acc is None else acc + part
            if after:
                after[i].start()
        res = acc.astype(BF16)
        x[pl.ds(r0, group), cols] = res
        for i in range(group // CAP):
            k = ROW_ORDER[r0 // CAP + i]
            if k == 0:
                back[pl.ds(0, CAP), cols] = res[i * CAP:(i + 1) * CAP]

    def give_back(n, r0, start=0, width=TN):
        for i in range(group // CAP):
            k = ROW_ORDER[r0 // CAP + i]
            if k:
                return_copy(k, n, start, width).start()

    send_copy(1).wait_recv()

    @pl.loop(0, SPLIT - 1)
    def _(j):
        wait_all(up_copies(j))
        up_tile(j, own, 0, group)

    for k in (2, 4):
        send_copy(k).wait_send()
    for k in (6, 7):
        send_copy(k).start()
    wait_all(up_copies(SPLIT - 1))
    up_tile(SPLIT - 1, own, 0, group)
    send_copy(2).wait_recv()
    send_copy(4).wait_recv()

    @pl.loop(SPLIT, n_ff)
    def _(j):
        wait_all(up_copies(j))
        up_tile(j, own, 0, 2 * group)

    def up_slots(slots):
        return [pltpu.make_async_copy((w3_hbm if p % 2 else w1_hbm).at[0, :, pl.ds((p // 2) * TN, TN)],
                                      pool.at[p], pool_sem.at[p]) for p in slots]

    rest = n_k - EXTRA

    def middle_copies(lent):
        return down_copies(1, lent[:rest], EXTRA) + down_copies(2, lent[rest:])

    def start_middle(lent):
        start_all(middle_copies(lent))

    def down_first(n, then, lent, r0):
        if r0 != near:
            wait_all(middle_copies(lent))
        after = None if then is None else down_copies(then, home)
        if r0 == far:
            for start in (0, TN // 2):
                acc = sum(dot(h[pl.ds(group, group), pl.ds(s, size)],
                              pool[home[i], pl.ds(0, size), pl.ds(start, TN // 2)]) for i, (s, size) in enumerate(kparts))
                x[pl.ds(r0, group), pl.ds(n * TN + start, TN // 2)] = acc.astype(BF16)
                if start:
                    start_all(after)
                give_back(n, r0, start, TN // 2)
        else:
            down_tile(n, home, r0, group, after)
            give_back(n, r0)
        if r0 == near:
            wait_all(middle_copies(lent))
        down_tile(1, extra + lent[:rest], r0, group)
        down_tile(2, lent[rest:], r0, group)
        for n in (1, 2):
            give_back(n, r0)

    n_lent = rest + n_k
    back_c = -(-n_lent // 2)
    lent_a = list(range(2 * n_ff - n_lent, 2 * n_ff))
    lent_b = list(range(0, n_lent))
    lent_c = list(range(2 * back_c, 2 * back_c + n_lent))
    last_c = list(range(lent_c[-1] + 1, lent_c[-1] + 1 + n_k))
    start_middle(lent_a)

    for j in range(SPLIT):
        up_tile(j, near, group, group)
    for k in (3, 5):
        send_copy(k).start()
    wait_all(down_copies(0, home) + down_copies(1, extra))
    down_first(0, 3, lent_a, near)
    start_all(up_slots(lent_a))
    wait_all(down_copies(3, home))
    down_tile(3, home, near, group)
    give_back(3, near)

    send_copy(6).wait_recv()
    send_copy(7).wait_recv()
    for j in range(0, 4):
        up_tile(j, far, group, group)
    start_middle(lent_b)
    for j in range(4, 8):
        up_tile(j, far, group, group)
    wait_all(up_slots(lent_a))
    for j in range(8, n_ff):
        up_tile(j, far, group, group)
    down_first(3, 0, lent_b, far)
    start_all(up_slots(lent_b))
    wait_all(down_copies(0, home))
    down_tile(0, home, far, group)
    give_back(0, far)

    send_copy(3).wait_recv()
    send_copy(5).wait_recv()
    for j in range(back_c, back_c + 4):
        up_tile(j, late, group, group)
    start_middle(lent_c)
    start_all(down_copies(3, last_c))
    for j in range(back_c + 4, n_ff):
        up_tile(j, late, group, group)
    wait_all(up_slots(lent_b))
    for j in range(back_c):
        up_tile(j, late, group, group)
    down_first(0, None, lent_c, late)
    wait_all(down_copies(3, last_c))
    down_tile(3, last_c, late, group)
    give_back(3, late)

    own_slots = (home, extra + lent_c[:rest], lent_c[rest:], last_c)
    for n in range(n_out):
        down_tile(n, own_slots[n], own, 0)
    for n in range(n_out):
        give_back(n, own)
    for k in range(1, N_DEV):
        if k not in (2, 4):
            send_copy(k).wait_send()

    pick = xsend.at[pl.ds(0, 2 * TOK), pl.ds(0, N_DEV * CAP)]
    wide = lax.broadcasted_iota(jnp.int32, (TOK, N_DEV * CAP), 1).astype(F32)
    for c in range(2):
        pick[pl.ds(c * TOK, TOK), :] = jnp.where(wide == gate[:, 2 + c:3 + c], 1.0, 0.0).astype(BF16)

    for tiles in ((0, 1), (2,), (3,)):
        for n in tiles:
            returned(n).wait_recv()
        for n in tiles:
            cols = pl.ds(n * TN, TN)
            both = dot(pick[...], back[:, cols])
            hid[:, cols] = (gate[:, 0:1] * both[:TOK] + gate[:, 1:2] * both[TOK:]).astype(BF16)
    for n in range(n_out):
        returned(n).wait_send()


def solution(mesh):
    def device_body(hidden, w_router, ids, w_one, w_three, w_two):
        d_model, ff = w_one.shape[1:]
        n_exp = w_router.shape[1]
        rows = N_DEV * CAP
        n_out = d_model // TN
        n_slots = 2 * (ff // TN) + -(-ff // d_model) + EXTRA
        dma = pltpu.SemaphoreType.DMA
        return pl.pallas_call(
            moe_kernel,
            out_shape=pltpu.VMEM(hidden.shape, BF16),
            in_specs=[pl.BlockSpec(memory_space=pl.ANY)] * 6,
            out_specs=pl.BlockSpec(memory_space=pltpu.VMEM),
            scratch_shapes=[
                pltpu.VMEM((n_exp, d_model), F32),
                pltpu.VMEM((2, TOK), jnp.int32),
                pltpu.VMEM((rows, d_model), BF16),
                pltpu.VMEM((5 * CAP, d_model), BF16),
                pltpu.VMEM((rows, d_model), BF16),
                pltpu.VMEM((2 * TOK, ff), BF16),
                pltpu.VMEM((n_slots, d_model, TN), BF16),
                pltpu.VMEM((n_exp, TOK), F32),
                pltpu.VMEM((TOK, N_DEV), F32),
                dma((3,)), dma((n_slots,)), dma((N_DEV,)), dma((N_DEV,)),
                dma((n_out,)), dma((n_out,)),
            ],
            compiler_params=pltpu.CompilerParams(
                collective_id=0, has_side_effects=True, vmem_limit_bytes=VMEM_BYTES - 2 * hidden.size),
        )(hidden, w_router.T, ids.T, w_one, w_three, w_two)

    return jax.shard_map(
        device_body, mesh=mesh,
        in_specs=(P("ep", None), P(None, None), P("ep", None), P("ep", None, None), P("ep", None, None), P("ep", None, None)),
        out_specs=P("ep", None), check_vma=False)
```
